512 devices in a mesh: tenant: 2 (over y), ctx: 32 (over z), head: 8 (over x, core).
Axes of the slice: x: 4, y: 2, z: 32, core: 2. Of those that a mesh axis runs over, the one named last changes fastest.
The devices are a block of a 4x8x32 slice.
Arguments:
- tokens: bfloat16 [16384, 4608], P(('tenant', 'ctx'), 'head'), parts along dimension 0, may hold values from -6 to 6
- query_frozen_matrix: bfloat16 [4608, 2048], P('ctx', 'head'), may hold values from -0.09375 to 0.09375
- key_weight: bfloat16 [4608, 1024], P('ctx', 'head'), may hold values from -0.09375 to 0.09375
- value_frozen_matrix: bfloat16 [4608, 1024], P('ctx', 'head'), may hold values from -0.09375 to 0.09375
- query_down: bfloat16 [9216, 16], P('tenant'), parts along dimension 0, may hold values from -0.09375 to 0.09375
- query_adapter_expand: bfloat16 [32, 2048], P('tenant', 'head'), parts along dimension 0, may hold values from -1.5 to 1.5
- value_down: bfloat16 [9216, 16], P('tenant'), parts along dimension 0, may hold values from -0.09375 to 0.09375
- value_adapter_expand: bfloat16 [32, 1024], P('tenant', 'head'), parts along dimension 0, may hold values from -1.5 to 1.5
- block_order: int32 [128], P('tenant'), parts along dimension 0, may hold values from 0 to 63, each once
- doc_starts: int32 [24], P('tenant'), parts along dimension 0, may hold values from 0 to 8191, as said below
- prompt_of: int32 [24], P('tenant'), parts along dimension 0, may hold values from 0 to 11, as said below
Outputs:
- attended: bfloat16 [16384, 2048], P(('tenant', 'ctx'), 'head'), parts along dimension 0
The draws below stay inside these ranges and needn't reach their ends.
There are 2 independent parts, one for each index of `tenant`. The reference program is written for one: setup_inputs(seed, part) draws one part's arguments, and reference() takes and returns one part's arrays. A program takes and returns all parts, laid end to end along the dimension named above; an argument that names none is the same for every part. Nothing has to cross between parts.
Inputs may be any that keep to these rules, and one draw needn't show every extreme that they name: `doc_starts`: strictly increasing with first entry 0; the segments come in 4 groups of three: a prompt, a chosen and a rejected response. `prompt_of`: for segment j = 3k it is j; for j = 3k + 1 it is 3k; for j = 3k + 2 it is 3k or j. `block_order`: each of 0 to 63 once.
All inputs are finite; a program needn't handle non-finite values.
Results may differ from the reference program's by a relative error of at most 0.012.
Values may be sent and summed in bfloat16 or wider, within the bound.
A program may use at most 64 MiB of HBM per device.

```python
import math
import jax
import jax.numpy as jnp
from jax import lax

D = 4608
HEADS = 16
KV_HEADS = 8
HD = 128
RANK = 16
PAIRS = 4
TOK_DEV = 256
TOKENS = 8192
SEGS = 12
BLOCKS = 64
N_CTX = 32


def draw_doc_starts(key, part):
    cuts = jax.random.permutation(jax.random.fold_in(key, 11), TOKENS - 1)[:SEGS - 1] + 1
    return jnp.concatenate([jnp.zeros((1,), jnp.int32), jnp.sort(cuts.astype(jnp.int32))])


def draw_prompt_of(key, part):
    flags = jax.random.randint(jax.random.fold_in(key, 23), (PAIRS,), 0, 2)
    seg_ids = jnp.arange(SEGS, dtype=jnp.int32)
    leading = 3 * (seg_ids // 3)
    within = seg_ids % 3
    reads = (within == 1) | (within == 2) & (flags[seg_ids // 3] == 1)
    return jnp.where(reads, leading, seg_ids).astype(jnp.int32)


def block_levels(stream_key, shape, shards, smallest, top_value):
    level, own = 1.0, jax.random.fold_in(stream_key, 6)
    for dim, blocks in shards:
        steps = jnp.exp(jax.random.uniform(jax.random.fold_in(own, dim), (blocks,), jnp.float32, smallest / len(shards), top_value / len(shards)))
        level = level * jnp.repeat(steps, shape[dim] // blocks).reshape([-1 if axis == dim else 1 for axis in range(len(shape))])
    return level


def bell_draw(key, extent, width, reach, cuts=(), held_as=jnp.bfloat16):
    values = jax.random.normal(key, extent, jnp.float32) * width
    if len(cuts) > 0:
        values = block_levels(key, extent, cuts, -0.22, 0.18) * values
    return jnp.clip(values, min=-reach, max=reach).astype(held_as)


def setup_inputs(seed: int = 0, part: int = 0) -> dict:
    key_of = jax.random.split(jax.random.key(seed), 12)
    part_keys = jax.random.split(jax.random.fold_in(key_of[11], part), 12)
    tokens = bell_draw(part_keys[0], (TOKENS, D), 1.0, 6.0, ((0, 32), (1, 8)))
    query_frozen_matrix = bell_draw(key_of[1], (D, HEADS * HD), D ** -0.5, 0.09375, ((0, 32), (1, 8)))
    key_weight = bell_draw(key_of[2], (D, KV_HEADS * HD), D ** -0.5, 0.09375, ((0, 32), (1, 8)))
    value_frozen_matrix = bell_draw(key_of[3], (D, KV_HEADS * HD), D ** -0.5, 0.09375, ((0, 32), (1, 8)))
    query_down = bell_draw(part_keys[4], (D, RANK), D ** -0.5, 0.09375)
    query_adapter_expand = bell_draw(part_keys[5], (RANK, HEADS * HD), RANK ** -0.5, 1.5, ((1, 8),))
    value_down = bell_draw(part_keys[6], (D, RANK), D ** -0.5, 0.09375)
    value_adapter_expand = bell_draw(part_keys[7], (RANK, KV_HEADS * HD), RANK ** -0.5, 1.5, ((1, 8),))
    block_order = jax.random.permutation(part_keys[8], BLOCKS).astype(jnp.int32)
    doc_starts = draw_doc_starts(jax.random.fold_in(jax.random.fold_in(key_of[11], part), 71), part)
    prompt_of = draw_prompt_of(jax.random.fold_in(jax.random.fold_in(key_of[11], part), 71), part)
    return {"tokens": tokens, "query_frozen_matrix": query_frozen_matrix, "key_weight": key_weight, "value_frozen_matrix": value_frozen_matrix, "query_down": query_down, "query_adapter_expand": query_adapter_expand, "value_down": value_down, "value_adapter_expand": value_adapter_expand, "block_order": block_order, "doc_starts": doc_starts, "prompt_of": prompt_of}


softcap_limit = 50.0
query_scale = 144.0 ** -0.5
adapter_scaling = 2.0
rope_base = 10000.0


def row_meta(row_ids, block_order, doc_starts, prompt_of, block_len, sequence_len):
    block_count = block_order.shape[0]
    block_id = row_ids // block_len
    one_hot = block_id[:, None] == jnp.arange(block_count, dtype=jnp.int32)[None, :]
    ordered = jnp.sum(jnp.where(one_hot, block_order[None, :], 0), axis=1).astype(jnp.int32)
    places = ordered * block_len + row_ids % block_len
    segment = jnp.sum((doc_starts[None, :] <= places[:, None]).astype(jnp.int32), axis=1) - 1
    seg_ids = jnp.arange(doc_starts.shape[0], dtype=jnp.int32)
    selected = segment[:, None] == seg_ids[None, :]
    prompt_seg = jnp.sum(jnp.where(selected, prompt_of[None, :], 0), axis=1).astype(jnp.int32)
    own_start = jnp.sum(jnp.where(selected, doc_starts[None, :], 0), axis=1).astype(jnp.int32)
    next_starts = jnp.concatenate([doc_starts[1:], jnp.full((1,), sequence_len, jnp.int32)])
    prompt_sel = prompt_seg[:, None] == seg_ids[None, :]
    prompt_len = jnp.sum(jnp.where(prompt_sel, (next_starts - doc_starts)[None, :], 0), axis=1).astype(jnp.int32)
    rotary_pos = places - own_start + jnp.where(prompt_seg != segment, prompt_len, 0)
    return places, segment, prompt_seg, rotary_pos


def rotate(values_in, rotary_pos):
    width_half = values_in.shape[-1] // 2
    frequency = jnp.exp(jnp.arange(width_half, dtype=jnp.float32) * (-2.0 * math.log(rope_base) / values_in.shape[-1]))
    angles = rotary_pos.astype(jnp.float32)[:, None] * frequency[None, :]
    cosine = jnp.concatenate([jnp.cos(angles), jnp.cos(angles)], axis=-1)[:, None, :]
    sine_part = jnp.concatenate([jnp.sin(angles), jnp.sin(angles)], axis=-1)[:, None, :]
    rotated = jnp.concatenate([-values_in[..., width_half:], values_in[..., :width_half]], axis=-1)
    return values_in * cosine + rotated * sine_part


def visible_mask(query_info, key_info):
    same_doc = (key_info[1][None, :] == query_info[1][:, None]) & (key_info[0][None, :] <= query_info[0][:, None])
    from_prompt = (key_info[1][None, :] == query_info[2][:, None]) & (query_info[2] != query_info[1])[:, None]
    return same_doc | from_prompt


def reference(tokens, query_frozen_matrix, key_weight, value_frozen_matrix, query_down, query_adapter_expand, value_down, value_adapter_expand, block_order, doc_starts, prompt_of):
    row_ids = jnp.arange(TOKENS, dtype=jnp.int32)
    row_info = row_meta(row_ids, block_order, doc_starts, prompt_of, TOK_DEV // 2, TOKENS)
    query_adapter_hidden = jnp.dot(tokens, query_down, preferred_element_type=jnp.float32).astype(jnp.bfloat16)
    query_states = jnp.dot(tokens, query_frozen_matrix, preferred_element_type=jnp.float32) + adapter_scaling * jnp.dot(query_adapter_hidden, query_adapter_expand, preferred_element_type=jnp.float32)
    query_states = (rotate(query_states.reshape(TOKENS, HEADS, HD), row_info[3]) * query_scale).astype(jnp.bfloat16)
    key_proj = jnp.dot(tokens, key_weight, preferred_element_type=jnp.float32).reshape(TOKENS, KV_HEADS, HD)
    key_proj = rotate(key_proj, row_info[3]).astype(jnp.bfloat16)
    value_adapter_hidden = jnp.dot(tokens, value_down, preferred_element_type=jnp.float32).astype(jnp.bfloat16)
    value_projected = jnp.dot(tokens, value_frozen_matrix, preferred_element_type=jnp.float32) + adapter_scaling * jnp.dot(value_adapter_hidden, value_adapter_expand, preferred_element_type=jnp.float32)
    value_projected = value_projected.astype(jnp.bfloat16).reshape(TOKENS, KV_HEADS, HD)
    per_kv = HEADS // KV_HEADS
    key_wide = key_proj.astype(jnp.float32)
    value_wide = value_projected.astype(jnp.float32)
    query_blocks = query_states.astype(jnp.float32).reshape(N_CTX, TOK_DEV, KV_HEADS, per_kv, HD)
    info_blocks = tuple(entry.reshape(N_CTX, TOK_DEV) for entry in row_info[:3])

    def one_block(inputs):
        query_block, places, segment, prompt_seg = inputs
        visible = visible_mask((places, segment, prompt_seg), row_info)
        scores = jnp.einsum("tkgd,skd->kgts", query_block, key_wide)
        capped = softcap_limit * jnp.tanh(scores / softcap_limit)
        unnorm = jnp.where(visible[None, None], jnp.exp(capped), jnp.zeros_like(capped))
        denominator = jnp.sum(unnorm, axis=-1)
        rounded = lax.optimization_barrier(unnorm.astype(jnp.bfloat16)).astype(jnp.float32)
        numerator = jnp.einsum("kgts,skd->tkgd", rounded, value_wide)
        return (numerator / jnp.transpose(denominator, (2, 0, 1))[..., None]).astype(jnp.bfloat16)

    blocks_out = lax.map(one_block, (query_blocks,) + info_blocks)
    return blocks_out.reshape(TOKENS, HEADS * HD)
```

```python
import functools
import math

import jax
import jax.numpy as jnp
from jax import lax
from jax.experimental import pallas as pl
from jax.experimental.pallas import tpu as pltpu
from jax.sharding import PartitionSpec as P

HD = 128
MESH = pl.DeviceIdType.MESH
softcap_limit = 50.0
query_scale = 144.0 ** (-0.5)
adapter_scaling = 2.0
rope_base = 10000.0
exp_scale = softcap_limit / math.log(2.0)


def dot(a, b):
    return jnp.dot(a, b, preferred_element_type=jnp.float32)


def dot_nt(a, b):
    return lax.dot_general(a, b, (((1,), (1,)), ((), ())), preferred_element_type=jnp.float32)


def kernel(
    n, heads, freq_ref, tok_ref, wq_ref, wk_ref, wv_ref, qd_ref, qe_ref, vd_ref, ve_ref,
    order_ref, starts_ref, prompt_ref, out_ref,
    tok_all, w_all, kv_all, low_q, low_v, acc_kv, acc_q, q_s, geo, cos_s, sin_s, num, den,
    t_send, t_recv, d_send, d_recv, w_send, w_recv, k_send, k_recv,
):
    me = lax.axis_index("ctx")
    head = lax.axis_index("head")
    rows, feat = tok_ref.shape
    depth = wq_ref.shape[0]
    half_steps = n // 2
    group = feat // depth
    chips = heads // 2
    segs = starts_ref.shape[0]
    block_len = rows // 2
    right = lax.rem(me + 1, n)
    left = lax.rem(me + n - 1, n)
    partner = head + 1 - 2 * lax.rem(head, 2)

    def same_core(step):
        return lax.rem(head + 2 * step, heads)

    barrier = pltpu.get_barrier_semaphore()
    for ctx in (left, right):
        pl.semaphore_signal(barrier, inc=1, device_id={"ctx": ctx}, device_id_type=MESH)
    pl.semaphore_signal(barrier, inc=1, device_id={"head": partner}, device_id_type=MESH)
    for k in range(1, chips):
        pl.semaphore_signal(barrier, inc=1, device_id={"head": same_core(k)}, device_id_type=MESH)
    pl.semaphore_wait(barrier, 3 + chips - 1)

    def weight_source(c):
        if c == 0:
            return wk_ref
        if c == 1:
            return wv_ref
        return wq_ref.at[:, pl.ds((c - 2) * HD, HD)]

    def block_at(d, step):
        return lax.rem(me + step, n) if d else lax.rem(me + n - step, n)

    def w_slot(c, block):
        return w_all.at[c, pl.ds(pl.multiple_of(block * depth, depth), depth)]

    def w_copy(d, step, c):
        block = block_at(d, step - 1)
        return pltpu.make_async_remote_copy(
            src_ref=weight_source(c) if step == 1 else w_slot(c, block),
            dst_ref=w_slot(c, block),
            send_sem=w_send.at[d, step - 1, c],
            recv_sem=w_recv.at[d, step - 1, c],
            device_id={"ctx": left if d else right},
            device_id_type=MESH,
        )

    def w_wait(d, step, c):
        slot = w_slot(c, block_at(d, step))
        pltpu.make_async_remote_copy(
            src_ref=slot, dst_ref=slot, send_sem=w_send.at[d, step - 1, c],
            recv_sem=w_recv.at[d, step - 1, c], device_id={"ctx": right}, device_id_type=MESH,
        ).wait_recv()

    def w_ways(step):
        if step < half_steps:
            return [(d, c) for c in range(4) for d in range(2)]
        return [(0, 0), (1, 2), (0, 1), (1, 3)]

    for d, c in w_ways(1):
        w_copy(d, 1, c).start()

    def t_copy(k):
        return pltpu.make_async_remote_copy(
            src_ref=tok_ref, dst_ref=tok_all.at[head], send_sem=t_send.at[k], recv_sem=t_recv.at[k],
            device_id={"head": same_core(k)}, device_id_type=MESH,
        )

    def t_wait(k):
        slot = tok_all.at[lax.rem(head + heads - 2 * k, heads)]
        pltpu.make_async_remote_copy(
            src_ref=slot, dst_ref=slot, send_sem=t_send.at[k], recv_sem=t_recv.at[k],
            device_id={"head": partner}, device_id_type=MESH,
        ).wait_recv()

    def d_copy(k):
        source = lax.rem(head + heads - 2 * k, heads)
        return pltpu.make_async_remote_copy(
            src_ref=tok_ref if k == 0 else tok_all.at[source], dst_ref=tok_all.at[source],
            send_sem=d_send.at[k], recv_sem=d_recv.at[k],
            device_id={"head": partner}, device_id_type=MESH,
        )

    def d_wait(k):
        slot = tok_all.at[lax.rem(partner + heads - 2 * k, heads)]
        pltpu.make_async_remote_copy(
            src_ref=slot, dst_ref=slot, send_sem=d_send.at[k], recv_sem=d_recv.at[k],
            device_id={"head": partner}, device_id_type=MESH,
        ).wait_recv()

    for k in range(1, chips):
        t_copy(k).start()
    d_copy(0).start()

    tok_all[head] = tok_ref[...]
    own = pl.ds(pl.multiple_of(me * depth, depth), depth)
    w_all[0, own] = wk_ref[...]
    w_all[1, own] = wv_ref[...]
    w_all[2, own] = wq_ref[:, :HD]
    w_all[3, own] = wq_ref[:, HD:]

    sequence_len = rows * n

    def geometry():
        place = lax.broadcasted_iota(jnp.int32, (block_len, HD), 0)
        for part in range(2):
            p = place + order_ref[2 * me + part] * block_len
            a = jnp.zeros_like(p)
            b = jnp.zeros_like(p)
            e = jnp.zeros_like(p)
            for j in range(segs):
                m = prompt_ref[j]
                reads = m != j
                stop = jnp.where(m + 1 < segs, starts_ref[jnp.minimum(m + 1, segs - 1)], sequence_len)
                begin = jnp.where(reads, starts_ref[m], 0)
                stop = jnp.where(reads, stop, 0)
                start = starts_ref[j]
                here = p >= start
                a = jnp.where(here, start, a)
                b = jnp.where(here, begin, b)
                e = jnp.where(here, stop, e)
            span = pl.ds(part * block_len, block_len)
            geo[0, span] = a
            geo[1, span] = p
            geo[2, span] = b
            geo[3, span] = e
            angle = (p - a + e - b).astype(jnp.float32) * freq_ref[...]
            lane = lax.broadcasted_iota(jnp.int32, (block_len, HD), 1)
            sine = jnp.sin(angle)
            cos_s[span] = jnp.cos(angle)
            sin_s[span] = jnp.where(lane < HD // 2, -sine, sine)

    def add_group(g, first=False):
        tok = tok_all[g]
        span = pl.ds(pl.multiple_of(g * feat, feat), feat)
        kv = dot(tok, jnp.concatenate([w_all[0, span], w_all[1, span]], axis=1))
        q = dot(tok, jnp.concatenate([w_all[2, span], w_all[3, span]], axis=1))
        if first:
            acc_kv[...] = kv
            acc_q[...] = q
        else:
            acc_kv[...] += kv
            acc_q[...] += q

    def add_low(h):
        span = pl.ds(h * feat, feat)
        tok = tok_all[h]
        q = dot_nt(tok, qd_ref[:, span])
        v = dot_nt(tok, vd_ref[:, span])
        if h == 0:
            low_q[...] = q
            low_v[...] = v
        else:
            low_q[...] += q
            low_v[...] += v

    forward_at = half_steps * 6 // 16
    arrive_at = half_steps * 9 // 16
    waiting = {}
    my_group = me // group
    for j in range(heads // 2 + 1):
        ready = min(group * j + group - 1, half_steps)
        gs = [my_group] if j == 0 else [lax.rem(my_group + j, heads)]
        if 0 < j < heads // 2:
            gs.append(lax.rem(my_group + heads - j, heads))
        for g in gs:
            waiting.setdefault(max(ready, arrive_at), []).append(g)
    queue = []
    low_left = list(range(heads))
    first = True
    for step in range(1, half_steps + 1):
        for d, c in w_ways(step):
            w_wait(d, step, c)
            if step < half_steps and (d, c) in w_ways(step + 1):
                w_copy(d, step + 1, c).start()
        if step == 1:
            geometry()
        if step == forward_at:
            for k in range(1, chips):
                t_wait(k)
                d_copy(k).start()
        if step == arrive_at:
            for k in range(chips):
                d_wait(k)
        queue += waiting.get(step, [])
        take = len(queue) if step == half_steps else 1
        for g in queue[:take]:
            add_group(g, first)
            first = False
        queue = queue[take:]
        if step > arrive_at:
            take = 2 if step < half_steps - 1 else len(low_left)
            for h in low_left[:take]:
                add_low(h)
            low_left = low_left[take:]

    def k_slot(c, block):
        return kv_all.at[c, pl.ds(pl.multiple_of(block * rows, rows), rows)]

    def rotated(x):
        return x * cos_s[...] + pltpu.roll(x, HD // 2, 1) * sin_s[...]

    own_rows = pl.ds(pl.multiple_of(me * rows, rows), rows)
    kv_all[0, own_rows] = rotated(acc_kv[:, :HD]).astype(jnp.bfloat16)
    low = low_v[...].astype(jnp.bfloat16)
    kv_all[1, own_rows] = (acc_kv[:, HD:] + adapter_scaling * dot(low, ve_ref[...])).astype(jnp.bfloat16)
    low = low_q[...].astype(jnp.bfloat16)
    q = acc_q[...] + adapter_scaling * dot(low, qe_ref[...])
    for i in range(2):
        q_s[i] = (rotated(q[:, i * HD:(i + 1) * HD]) * query_scale).astype(jnp.bfloat16)

    def k_copy(d, step, c):
        block = block_at(d, step - 1)
        slot = k_slot(c, block)
        return pltpu.make_async_remote_copy(
            src_ref=slot, dst_ref=slot,
            send_sem=k_send.at[d, step - 1, c], recv_sem=k_recv.at[d, step - 1, c],
            device_id={"ctx": left if d else right}, device_id_type=MESH,
        )

    def k_wait(d, step, c):
        slot = k_slot(c, block_at(d, step))
        pltpu.make_async_remote_copy(
            src_ref=slot, dst_ref=slot, send_sem=k_send.at[d, step - 1, c],
            recv_sem=k_recv.at[d, step - 1, c], device_id={"ctx": right}, device_id_type=MESH,
        ).wait_recv()

    for c in range(2):
        for d in range(2):
            k_copy(d, 1, c).start()

    def attend(block, first=False):
        span = pl.ds(pl.multiple_of(block * rows, rows), rows)
        keys = kv_all[0, span]
        values = kv_all[1, span]
        lane = lax.broadcasted_iota(jnp.int32, (8, block_len), 1)
        places = [lane + order_ref[2 * block + part] * block_len for part in range(2)]
        tile = block_len
        for t in range(2):
            r = pl.ds(t * tile, tile)
            a, p, b, e = (geo[k, r].reshape(tile // 8, 8, HD) for k in range(4))
            visible = []
            for place in places:
                c = place[None]
                seen = ((c >= a) & (c <= p)) | ((c >= b) & (c < e))
                visible.append(seen.reshape(tile, HD))
            for i in range(2):
                s = dot_nt(q_s[i, r], keys)
                w = jnp.exp2(jnp.tanh(s * (1.0 / softcap_limit)) * exp_scale)
                w0 = jnp.where(visible[0], w[:, :HD], 0.0)
                w1 = jnp.where(visible[1], w[:, HD:], 0.0)
                total = dot(jnp.concatenate([w0.astype(jnp.bfloat16), w1.astype(jnp.bfloat16)], axis=1), values)
                if first:
                    den[i, r] = w0 + w1
                    num[i, r] = total
                else:
                    den[i, r] += w0 + w1
                    num[i, r] += total

    attend(me, True)

    def k_step(step, carry):
        for c in range(2):
            for d in range(2):
                k_wait(d, step, c)
                k_copy(d, step + 1, c).start()
        attend(block_at(0, step))
        attend(block_at(1, step))
        return carry

    lax.fori_loop(1, half_steps - 1, k_step, 0)
    step = half_steps - 1
    for c in range(2):
        for d in range(2):
            k_wait(d, step, c)
            if c == d:
                k_copy(d, step + 1, c).start()
    attend(block_at(0, step))
    attend(block_at(1, step))
    for c in range(2):
        k_wait(c, half_steps, c)
    attend(block_at(0, half_steps))

    for i in range(2):
        total = jnp.sum(den[i], axis=1, keepdims=True)
        out_ref[:, i * HD:(i + 1) * HD] = (num[i] / total).astype(jnp.bfloat16)

    for k in range(1, chips):
        t_copy(k).wait_send()
    for k in range(chips):
        d_copy(k).wait_send()
    for step in range(1, half_steps + 1):
        for d, c in w_ways(step):
            w_copy(d, step, c).wait_send()

    def k_sent(step, carry):
        for c in range(2):
            for d in range(2):
                k_copy(d, step, c).wait_send()
        return carry

    lax.fori_loop(1, half_steps, k_sent, 0)
    for c in range(2):
        k_copy(c, half_steps, c).wait_send()


def local(n, heads, tokens, wq, wk, wv, qd, qe, vd, ve, order, starts, prompts):
    rows, feat = tokens.shape
    depth = wq.shape[0]
    half = HD // 2
    lanes = jnp.arange(half, dtype=jnp.float32)
    freq = jnp.exp(lanes * (-2.0 * math.log(rope_base) / HD))
    freq = jnp.concatenate([freq, freq])[None, :]
    vmem = pl.BlockSpec(memory_space=pltpu.VMEM)
    smem = pl.BlockSpec(memory_space=pltpu.SMEM)
    bf16, f32 = jnp.bfloat16, jnp.float32
    dma = pltpu.SemaphoreType.DMA
    steps = n // 2
    return pl.pallas_call(
        functools.partial(kernel, n, heads),
        out_shape=jax.ShapeDtypeStruct((rows, wq.shape[1]), bf16),
        in_specs=[vmem] * 9 + [smem] * 3,
        out_specs=vmem,
        scratch_shapes=[
            pltpu.VMEM((heads, rows, feat), bf16),
            pltpu.VMEM((4, n * depth, HD), bf16),
            pltpu.VMEM((2, n * rows, HD), bf16),
            pltpu.VMEM((rows, qd.shape[1]), f32),
            pltpu.VMEM((rows, vd.shape[1]), f32),
            pltpu.VMEM((rows, 2 * HD), f32),
            pltpu.VMEM((rows, 2 * HD), f32),
            pltpu.VMEM((2, rows, HD), bf16),
            pltpu.VMEM((4, rows, HD), jnp.int32),
            pltpu.VMEM((rows, HD), f32),
            pltpu.VMEM((rows, HD), f32),
            pltpu.VMEM((2, rows, HD), f32),
            pltpu.VMEM((2, rows, HD), f32),
            dma((heads // 2,)), dma((heads // 2,)), dma((heads // 2,)), dma((heads // 2,)),
            dma((2, steps, 4)), dma((2, steps, 4)),
            dma((2, steps, 2)), dma((2, steps, 2)),
        ],
        compiler_params=pltpu.CompilerParams(
            collective_id=0, has_side_effects=True, vmem_limit_bytes=48 * 1024 * 1024
        ),
    )(freq, tokens, wq, wk, wv, qd.T, qe, vd.T, ve, order, starts, prompts)


def solution(mesh):
    n, heads = mesh.shape["ctx"], mesh.shape["head"]
    in_specs = (
        P(("tenant", "ctx"), "head"),
        P("ctx", "head"),
        P("ctx", "head"),
        P("ctx", "head"),
        P("tenant", None),
        P("tenant", "head"),
        P("tenant", None),
        P("tenant", "head"),
        P("tenant"),
        P("tenant"),
        P("tenant"),
    )
    out_specs = P(("tenant", "ctx"), "head")
    return jax.shard_map(
        functools.partial(local, n, heads), mesh=mesh, in_specs=in_specs, out_specs=out_specs, check_vma=False
    )
```
